256 devices in a mesh: groups: 2 (over z), expert: 128 (over y, x, core).
Axes of the slice: x: 8, y: 8, z: 2, core: 2. Of those that a mesh axis runs over, the one named last changes fastest.
The devices are a block of a 8x8x16 slice.
Arguments:
- tokens: bfloat16 [2048, 4096], P(('groups', 'expert')), parts along dimension 0, may hold values from -400 to 400
- norm_gain: float32 [4096], replicated, may hold values from 0.1 to 1.9
- expert_ids: int32 [2048, 8], P(('groups', 'expert')), parts along dimension 0, may hold values from 0 to 63, all different within a row; in each aligned block of 8 rows (0 to 7, 8 to 15, ...) at most 2 rows name the same one
- route_score: float32 [2048, 8], P(('groups', 'expert')), parts along dimension 0, may hold values from 0.05 to 1
- expert_pair: int32 [128], P('groups'), parts along dimension 0, may hold values from 0 to 63, each once
- w_in: bfloat16 [256, 4096, 768], P(('groups', 'expert')), parts along dimension 0, may hold values from -0.09375 to 0.09375
- w_out: bfloat16 [256, 384, 4096], P(('groups', 'expert')), parts along dimension 0, may hold values from -0.4375 to 0.4375
Outputs:
- mixed: bfloat16 [2048, 4096], P(('groups', 'expert')), parts along dimension 0
The draws below stay inside these ranges and needn't reach their ends.
There are 2 independent parts, one for each index of `groups`. The reference program is written for one: setup_inputs(seed, part) draws one part's arguments, and reference() takes and returns one part's arrays. A program takes and returns all parts, laid end to end along the dimension named above; an argument that names none is the same for every part. Nothing has to cross between parts.
Inputs may be any that keep to these rules, and one draw needn't show every extreme that they name: `expert_ids`: each token names 8 different experts; among the tokens of one device no expert is named by more than 2 tokens, and in some devices' tokens one expert is named by exactly 2. `expert_pair`: each value once.
All inputs are finite; a program needn't handle non-finite values.
Results may differ from the reference program's by a relative error of at most 0.0076.
Values may be sent and summed in bfloat16 or wider, within the bound.
A program may use at most 64 MiB of HBM per device.

```python
import math
import jax
import jax.numpy as jnp
import numpy as np
from jax import lax

D = 4096
EXPERT_FF = 768
TOP = 8
TOK_DEV = 8
HALF_FF = 384
EXPERTS = 64
TOKENS = 1024
CAP = 2
N_EXPERT = 128


def draw_tokens(key, part):
    first, second, third = jax.random.split(key, 3)
    base = jnp.clip(jax.random.normal(first, (TOKENS, D), jnp.float32), -6.0, 6.0)
    scales = jnp.exp(jax.random.uniform(second, (TOKENS, 1), jnp.float32, 0.0, math.log(10.0)))
    columns = jnp.exp(jax.random.uniform(third, (1, D), jnp.float32, math.log(0.3), math.log(3.0)))
    return (base * scales * columns).astype(jnp.bfloat16)


def steps_of(key, extent, cuts, smallest, largest):
    gain, own = 1.0, jax.random.fold_in(key, 6)
    for dim, shards_of in cuts:
        draws = jnp.exp(jax.random.uniform(jax.random.fold_in(own, dim), (shards_of,), jnp.float32, smallest / len(cuts), largest / len(cuts)))
        gain = gain * jnp.repeat(draws, extent[dim] // shards_of).reshape([-1 if axis == dim else 1 for axis in range(len(extent))])
    return gain


def shared_out(rng, own, number, rows, amount, top, most, slope):
    ranking = jax.random.permutation(rng, amount)
    crowded, ordinary = portions_of(amount, rows * top, most, slope, True), portions_of(amount, rows * top, most, slope, False)
    places = jnp.arange(amount)

    def named(lengths, turn):
        used = int((lengths > 0).sum())
        fixed = max(1, used // 4)
        moved = fixed + (places - fixed + turn * (used - fixed)) % max(1, amount - fixed)
        return jnp.zeros((amount,), jnp.int32).at[ranking[jnp.where(places < fixed, places, moved)]].set(jnp.asarray(lengths, jnp.int32))

    lengths = jnp.where(number % 4 == 0, named(crowded, number // 4), named(ordinary, number - number // 4 - 1))
    mixed = jax.random.permutation(jax.random.fold_in(own, 3), amount)
    source_of, taker = mixed[0:amount // 2 * 2:2], mixed[1:amount // 2 * 2:2]
    room = jnp.minimum(lengths[source_of] - 1, most - lengths[taker]) // 2
    room = jnp.where((source_of == ranking[0]) | (taker == ranking[0]) | (lengths[taker] == 0), 0, jnp.maximum(room, 0))
    moved = jax.random.randint(jax.random.fold_in(own, 4), (amount // 2,), 0, 1 << 20) % (room + 1)
    lengths = lengths.at[source_of].add(-moved).at[taker].add(moved)
    items = jnp.searchsorted(jnp.cumsum(lengths), jnp.arange(rows * top), side="right").astype(jnp.int32)
    grid = items.reshape(top, rows).T
    grid = grid[jax.random.permutation(jax.random.fold_in(own, 1), rows)]
    turn = jax.random.randint(jax.random.fold_in(own, 2), (rows, 1), 0, top)
    return jnp.take_along_axis(grid, (jnp.arange(top)[None, :] + turn) % top, axis=1)


def portions_of(amount, total, bound, lean, full):
    weights = [(1 << 20) // math.isqrt(grade ** lean) + 1 for grade in range(1, amount + 1)]
    largest = bound if full else min(bound, max(-(-total // amount), total * weights[0] // sum(weights)))
    least = 1 if total - largest >= amount - 1 else 0
    given, spare = [largest] + [least] * (amount - 1), total - largest - least * (amount - 1)
    while spare > 0:
        movable = [i for i in range(1, amount) if given[i] < largest] or [i for i in range(1, amount) if given[i] < bound]
        whole, budget = sum([weights[i] for i in movable]), spare
        for i in movable:
            addition = min(bound - given[i], max(1, budget * weights[i] // whole), spare)
            given[i] = given[i] + addition
            spare = spare - addition
    return np.array(given)


def centred(key, extent, width, limit, cuts=(), kind=jnp.bfloat16):
    array = width * jax.random.normal(key, extent, jnp.float32)
    if cuts:
        array = array * steps_of(key, extent, cuts, -0.22, 0.18)
    return jnp.clip(array, -limit, limit).astype(kind)


def setup_inputs(seed: int = 0, part: int = 0) -> dict:
    key_of = jax.random.split(jax.random.key(seed), 8)
    part_splits = jax.random.split(jax.random.fold_in(key_of[7], part), 8)
    tokens = draw_tokens(jax.random.fold_in(jax.random.fold_in(key_of[7], part), 71), part)
    norm_gain = jnp.clip(1.0 + 0.18 * jax.random.normal(key_of[1], (D,), jnp.float32), 0.1, 1.9)
    expert_ids_keys = jax.random.split(jax.random.fold_in(part_splits[2], 1), TOKENS // TOK_DEV)
    expert_ids_turns = jax.random.permutation(jax.random.fold_in(part_splits[2], 3), TOKENS // TOK_DEV)
    expert_ids = jax.vmap(lambda own, number: shared_out(jax.random.fold_in(part_splits[2], 2), own, number, TOK_DEV, EXPERTS, TOP, CAP, 2))(expert_ids_keys, expert_ids_turns).reshape((TOKENS, TOP))
    route_score = jnp.clip(jnp.exp(math.log(1.0) - 2.9957323 * jax.random.uniform(part_splits[3], (TOKENS, TOP), jnp.float32) ** steps_of(part_splits[3], (TOKENS, TOP), ((0, 128),), -0.2, 0.2)), 0.05, 1.0)
    expert_pair = jax.random.permutation(part_splits[4], EXPERTS).astype(jnp.int32)
    w_in = centred(part_splits[5], (N_EXPERT, D, 2 * HALF_FF), D ** -0.5, 0.09375, ((0, 128),))
    w_out = centred(part_splits[6], (N_EXPERT, HALF_FF, D), (EXPERT_FF // 4) ** -0.5, 0.4375, ((0, 128),))
    return dict(tokens=tokens, norm_gain=norm_gain, expert_ids=expert_ids, route_score=route_score, expert_pair=expert_pair, w_in=w_in, w_out=w_out)


def reference(tokens, norm_gain, expert_ids, route_score, expert_pair, w_in, w_out):
    widened = tokens.astype(jnp.float32)
    meansq = lax.optimization_barrier(jnp.mean(widened * widened, axis=-1, keepdims=True))
    normed = (widened * lax.rsqrt(meansq + 1e-06) * norm_gain).astype(jnp.bfloat16)
    shares = (route_score / lax.optimization_barrier(jnp.sum(route_score, axis=-1, keepdims=True))).astype(jnp.bfloat16)
    half_units = w_out.shape[1]
    row_limit = N_EXPERT * CAP
    labels = jnp.arange(EXPERTS, dtype=jnp.int32)

    def expert_step(totals, expert):
        station = jnp.sum(jnp.where(labels == expert, expert_pair, 0)).astype(jnp.int32)
        inward = lax.dynamic_slice_in_dim(w_in, 2 * station, 2, 0)
        outward = lax.dynamic_slice_in_dim(w_out, 2 * station, 2, 0).reshape(2 * half_units, D)
        gate_full = jnp.concatenate([inward[0, :, :half_units], inward[1, :, :half_units]], axis=1)
        up_full = jnp.concatenate([inward[0, :, half_units:], inward[1, :, half_units:]], axis=1)
        chosen = expert_ids == expert
        members = jnp.nonzero(jnp.any(chosen, axis=-1), size=row_limit, fill_value=TOKENS)[0].astype(jnp.int32)
        inputs = jnp.take(normed, members, axis=0, mode='fill', fill_value=0)
        gate_val = jnp.dot(inputs, gate_full, preferred_element_type=jnp.float32)
        up_val = jnp.dot(inputs, up_full, preferred_element_type=jnp.float32)
        hidden = (jax.nn.silu(gate_val) * up_val).astype(jnp.bfloat16)
        result = jnp.dot(hidden, outward, preferred_element_type=jnp.float32).astype(jnp.bfloat16)
        token_weight = lax.optimization_barrier(jnp.sum(jnp.where(chosen, shares.astype(jnp.float32), 0.0), axis=-1))
        row_weight = jnp.take(token_weight, members, mode='fill', fill_value=0)
        totals = totals.at[members].add(row_weight[:, None] * result.astype(jnp.float32), mode='drop')
        return (totals, None)
    totals = lax.scan(expert_step, jnp.zeros((TOKENS, D), jnp.float32), labels)[0]
    return totals.astype(jnp.bfloat16)
```

```python
import functools

import jax
import jax.numpy as jnp
from jax import lax
from jax.experimental import pallas as pl
from jax.experimental.pallas import tpu as pltpu
from jax.sharding import Mesh
from jax.sharding import PartitionSpec as P

MESH = pl.DeviceIdType.MESH
GROUPS_EXPERT = ("groups", "y", "x", "core")
SLOTS = 2
LANES = 128
HALF_LANES = 64
CHUNKS = 4
F32 = jnp.float32
BF16 = jnp.bfloat16


def across(a, b):
    return lax.dot_general(a, b, (((1,), (1,)), ((), ())), preferred_element_type=F32)


def kernel(
    n, tokens, gain, ids, score, pair, w_in, w_out, out,
    win_v, wout_v, x, meta, g, a, acc, own, other, came, done, back, sums, last,
    win_sem, wout_sem, m_send, m_recv, s1, r1, s2, r2, s3, r3, s4, r4, sa, ra, sb, rb,
):
    y, col, core = lax.axis_index("y"), lax.axis_index("x"), lax.axis_index("core")
    first = y * (1 - core) + col * core
    second = col * (1 - core) + y * core

    def at(i, j):
        return {"y": i * (1 - core) + j * core, "x": j * (1 - core) + i * core, "core": core}

    partner = {"core": 1 - core}
    count, width = tokens.shape
    half = width // 2
    w = half // CHUNKS
    block = 2 * count
    group = n * SLOTS
    rows = n * block
    slots = n * group
    units = w_out.shape[1]

    weight_copies = []
    for k in range(CHUNKS):
        for h in range(2):
            weight_copies.append(pltpu.make_async_copy(
                w_in.at[0, pl.ds(h * half + k * w, w), :], win_v.at[k, pl.ds(h * w, w), :], win_sem.at[k, h]))
    for k in range(CHUNKS):
        for h in range(2):
            weight_copies.append(pltpu.make_async_copy(
                w_out.at[0, :, pl.ds(h * half + k * w, w)], wout_v.at[k, :, pl.ds(h * w, w)], wout_sem.at[k, h]))

    barrier = pltpu.get_barrier_semaphore()
    for d in range(1, n):
        pl.semaphore_signal(barrier, inc=1, device_id=at((first + d) % n, second), device_id_type=MESH)
        pl.semaphore_signal(barrier, inc=1, device_id=at(first, (second + d) % n), device_id_type=MESH)
    pl.semaphore_signal(barrier, inc=1, device_id=partner, device_id_type=MESH)
    for copy in weight_copies:
        copy.start()

    mine = pl.ds(pl.multiple_of(first * block, block), block)
    wide = tokens[...].astype(F32)
    scale = lax.rsqrt(jnp.mean(wide * wide, axis=-1, keepdims=True) + 1e-06)
    normed = wide * scale * gain[...]
    x[mine, :] = jnp.concatenate([normed[:, :half], normed[:, half:]], axis=0).astype(BF16)

    scores = score[...]
    shares = (scores / jnp.sum(scores, axis=-1, keepdims=True)).astype(BF16).astype(F32)
    named = ids[...]
    lane = lax.broadcasted_iota(jnp.int32, (count, LANES), 1)
    table = jnp.zeros((count, LANES), F32)
    for k in range(named.shape[1]):
        table = table + jnp.where(lane == named[:, k:k + 1], 1.0, 0.0)
        table = table + jnp.where(lane == named[:, k:k + 1] + HALF_LANES, shares[:, k:k + 1], 0.0)
    place = lax.broadcasted_iota(jnp.int32, (LANES, LANES), 0)
    table = across(table.astype(BF16), jnp.where(place == pair[...], 1.0, 0.0).astype(BF16))
    row = lax.broadcasted_iota(jnp.int32, (count, LANES), 0)
    earlier = jnp.zeros((count, LANES), F32)
    for t in range(count - 1):
        earlier = earlier + jnp.where(row > t, table[t:t + 1, :], 0.0)
    table = jnp.where(lane < HALF_LANES, table * (1.0 + earlier), table)
    meta[mine, :] = jnp.concatenate([table, table], axis=0).astype(BF16)

    pl.semaphore_wait(barrier, 2 * (n - 1) + 1)

    def send_meta(d):
        return pltpu.make_async_remote_copy(
            src_ref=meta.at[mine, :], dst_ref=meta.at[mine, :], send_sem=m_send.at[d], recv_sem=m_recv.at[d],
            device_id=at((first + d) % n, second), device_id_type=MESH)

    def send_x(k, d):
        part = pl.ds(k * w, w)
        return pltpu.make_async_remote_copy(
            src_ref=x.at[mine, part], dst_ref=x.at[mine, part], send_sem=s1.at[k, d], recv_sem=r1.at[k, d],
            device_id=at((first + d) % n, second), device_id_type=MESH)

    def group_of(j):
        return pl.ds(pl.multiple_of(j * group, group), group)

    def block_of(i):
        return pl.ds(pl.multiple_of(i * block, block), block)

    def send_slots(k, d):
        to = (second + d) % n
        return pltpu.make_async_remote_copy(
            src_ref=g.at[k, group_of(to), :], dst_ref=a.at[k, group_of(second), :],
            send_sem=s2.at[k, d], recv_sem=r2.at[k, d], device_id=at(first, to), device_id_type=MESH)

    def swap_rows(k):
        return pltpu.make_async_remote_copy(
            src_ref=a.at[k, pl.ds(0, slots), :], dst_ref=a.at[k, pl.ds(slots, slots), :],
            send_sem=sa.at[k], recv_sem=ra.at[k], device_id=partner, device_id_type=MESH)

    def swap_partial(k):
        return pltpu.make_async_remote_copy(
            src_ref=other.at[k], dst_ref=came.at[k],
            send_sem=sb.at[k], recv_sem=rb.at[k], device_id=partner, device_id_type=MESH)

    def send_back(k, d):
        to = (second + d) % n
        return pltpu.make_async_remote_copy(
            src_ref=done.at[k, group_of(to), :], dst_ref=back.at[k, group_of(second), :],
            send_sem=s3.at[k, d], recv_sem=r3.at[k, d], device_id=at(first, to), device_id_type=MESH)

    def send_sums(k, d):
        to = (first + d) % n
        return pltpu.make_async_remote_copy(
            src_ref=sums.at[k, block_of(to), :], dst_ref=last.at[k, block_of(first), :],
            send_sem=s4.at[k, d], recv_sem=r4.at[k, d], device_id=at(to, second), device_id_type=MESH)

    for d in range(1, n):
        send_meta(d).start()
    for k in range(CHUNKS):
        for d in range(1, n):
            send_x(k, d).start()

    for d in range(1, n):
        send_meta(d).wait_recv()
    stride = 1 + (n - 1) * core
    start = first * (n * (1 - core) + core)
    slot_a = lax.broadcasted_iota(jnp.int32, (slots, LANES), 0)
    lane_a = lax.broadcasted_iota(jnp.int32, (slots, LANES), 1)
    station = slot_a // group * stride + start
    choose = jnp.where(lane_a == station, 1.0, 0.0).astype(BF16)
    weigh = jnp.where(lane_a == station + HALF_LANES, 1.0, 0.0).astype(BF16)
    everything = meta[...]
    slot_s = lax.broadcasted_iota(jnp.int32, (slots, rows), 0)
    row_s = lax.broadcasted_iota(jnp.int32, (slots, rows), 1)
    hit = (across(choose, everything) == (slot_s % SLOTS + 1).astype(F32)) & (
        slot_s % group // SLOTS == row_s // block)
    picks = [jnp.where(hit & (row_s % block // count == h), 1.0, 0.0).astype(BF16) for h in range(2)]
    row_t = lax.broadcasted_iota(jnp.int32, (rows, slots), 0)
    slot_t = lax.broadcasted_iota(jnp.int32, (rows, slots), 1)
    hit_t = (across(everything, choose) == (slot_t % SLOTS + 1).astype(F32)) & (
        slot_t % group // SLOTS == row_t // block)
    share_t = across(everything, weigh)
    mixes = [jnp.where(hit_t & (row_t % block // count == h), share_t, 0.0).astype(BF16) for h in range(2)]

    def pick(k):
        for d in range(1, n):
            send_x(k, d).wait_recv()
        chunk = x[:, k * w:(k + 1) * w]
        for h in range(2):
            g[k, :, h * w:(h + 1) * w] = jnp.dot(picks[h], chunk, preferred_element_type=F32).astype(BF16)
        for d in range(1, n):
            send_slots(k, d).start()
        a[k, group_of(second), :] = g[k, group_of(second), :]

    def swap(k):
        for d in range(1, n):
            send_slots(k, d).wait_recv()
        swap_rows(k).start()

    def expand(k):
        for h in range(2):
            weight_copies[2 * k + h].wait()
        swap_rows(k).wait_recv()
        product = jnp.dot(a[k], win_v[k], preferred_element_type=F32)
        if k == 0:
            acc[...] = product
        else:
            acc[...] += product

    for stage, k in in_waves((pick, swap, expand), CHUNKS):
        stage(k)

    gate = acc[:, :units]
    hidden = (gate / (1.0 + jnp.exp(-gate)) * acc[:, units:]).astype(BF16)

    def contract(k):
        for h in range(2):
            weight_copies[2 * CHUNKS + 2 * k + h].wait()
        product = jnp.dot(hidden, wout_v[k], preferred_element_type=F32)
        other[k] = product[slots:].astype(BF16)
        own[k] = product[:slots]
        swap_partial(k).start()

    def finish(k):
        swap_partial(k).wait_recv()
        done[k] = (own[k] + came[k].astype(F32)).astype(BF16)
        for d in range(1, n):
            send_back(k, d).start()
        back[k, group_of(second), :] = done[k, group_of(second), :]

    def mix(k):
        for d in range(1, n):
            send_back(k, d).wait_recv()
        total = jnp.dot(mixes[0], back[k, :, :w], preferred_element_type=F32)
        total = total + jnp.dot(mixes[1], back[k, :, w:], preferred_element_type=F32)
        sums[k] = total.astype(BF16)
        for d in range(1, n):
            send_sums(k, d).start()
        last[k, block_of(first), :] = sums[k, block_of(first), :]

    def gather(k):
        for d in range(1, n):
            send_sums(k, d).wait_recv()
        total = last[k, 0:block, :].astype(F32)
        for i in range(1, n):
            total = total + last[k, i * block:(i + 1) * block, :].astype(F32)
        for h in range(2):
            out[:, h * half + k * w:h * half + (k + 1) * w] = total[h * count:(h + 1) * count].astype(BF16)

    for stage, k in in_waves((contract, finish, mix, gather), CHUNKS):
        stage(k)

    for d in range(1, n):
        send_meta(d).wait_send()
    for k in range(CHUNKS):
        swap_rows(k).wait_send()
        swap_partial(k).wait_send()
        for d in range(1, n):
            send_x(k, d).wait_send()
            send_slots(k, d).wait_send()
            send_back(k, d).wait_send()
            send_sums(k, d).wait_send()


def in_waves(stages, chunks):
    return [
        (stages[s], wave - s)
        for wave in range(len(stages) + chunks - 1)
        for s in range(len(stages))
        if 0 <= wave - s < chunks
    ]


def on_device(tokens, norm_gain, expert_ids, route_score, expert_pair, w_in, w_out):
    n = lax.axis_size("y")
    count, width = tokens.shape
    units = w_out.shape[1]
    w = width // 2 // CHUNKS
    rows, slots = n * 2 * count, n * n * SLOTS
    pair = jnp.full((LANES,), -1, jnp.int32)
    pair = pair.at[:expert_pair.shape[0]].set(expert_pair)
    pair = pair.at[HALF_LANES:HALF_LANES + expert_pair.shape[0]].set(expert_pair + HALF_LANES)
    vmem = pl.BlockSpec(memory_space=pltpu.VMEM)
    hbm = pl.BlockSpec(memory_space=pl.ANY)
    dma = pltpu.SemaphoreType.DMA
    return pl.pallas_call(
        functools.partial(kernel, n),
        out_shape=jax.ShapeDtypeStruct((count, width), BF16),
        in_specs=[vmem] * 5 + [hbm] * 2,
        out_specs=vmem,
        scratch_shapes=[
            pltpu.VMEM((CHUNKS, 2 * w, 2 * units), BF16),
            pltpu.VMEM((CHUNKS, units, 2 * w), BF16),
            pltpu.VMEM((rows, width // 2), BF16),
            pltpu.VMEM((rows, LANES), BF16),
            pltpu.VMEM((CHUNKS, slots, 2 * w), BF16),
            pltpu.VMEM((CHUNKS, 2 * slots, 2 * w), BF16),
            pltpu.VMEM((2 * slots, 2 * units), F32),
            pltpu.VMEM((CHUNKS, slots, 2 * w), F32),
            pltpu.VMEM((CHUNKS, slots, 2 * w), BF16),
            pltpu.VMEM((CHUNKS, slots, 2 * w), BF16),
            pltpu.VMEM((CHUNKS, slots, 2 * w), BF16),
            pltpu.VMEM((CHUNKS, slots, 2 * w), BF16),
            pltpu.VMEM((CHUNKS, rows, w), BF16),
            pltpu.VMEM((CHUNKS, rows, w), BF16),
            dma((CHUNKS, 2)), dma((CHUNKS, 2)), dma((n,)), dma((n,)),
            dma((CHUNKS, n)), dma((CHUNKS, n)), dma((CHUNKS, n)), dma((CHUNKS, n)),
            dma((CHUNKS, n)), dma((CHUNKS, n)), dma((CHUNKS, n)), dma((CHUNKS, n)),
            dma((CHUNKS,)), dma((CHUNKS,)), dma((CHUNKS,)), dma((CHUNKS,)),
        ],
        compiler_params=pltpu.CompilerParams(
            collective_id=0, has_side_effects=True, vmem_limit_bytes=48 << 20
        ),
    )(
        tokens, norm_gain.reshape(1, width), expert_ids, route_score, pair.reshape(1, LANES), w_in, w_out
    )


def solution(mesh):
    split = Mesh(mesh.devices.reshape(mesh.shape["groups"], 8, 8, 2), GROUPS_EXPERT)
    placed = (
        P(GROUPS_EXPERT, None),
        P(),
        P(GROUPS_EXPERT, None),
        P(GROUPS_EXPERT, None),
        P("groups"),
        P(GROUPS_EXPERT, None, None),
        P(GROUPS_EXPERT, None, None),
    )
    return jax.shard_map(
        on_device, mesh=split, in_specs=placed, out_specs=P(GROUPS_EXPERT, None), check_vma=False
    )
```

```python
import functools

import jax
import jax.numpy as jnp
from jax import lax
from jax.experimental import pallas as pl
from jax.experimental.pallas import tpu as pltpu
from jax.sharding import Mesh
from jax.sharding import PartitionSpec as P

MESH = pl.DeviceIdType.MESH
GROUPS_EXPERT = ("groups", "y", "x", "core")
SLOTS = 2
LANES = 128
HALF_LANES = 64
CHUNKS = 2
BATCHES = 2
F32 = jnp.float32
BF16 = jnp.bfloat16


def across(a, b):
    return lax.dot_general(a, b, (((1,), (1,)), ((), ())), preferred_element_type=F32)


def near_first(n):
    return sorted(range(n), key=lambda d: (min(d, n - d), d))


def kernel(
    n, tokens_in, gain_in, ids_in, score_in, pair_in, w_in, w_out, out,
    tokens, gain, ids, score, pair,
    win_v, wout_v, x, meta, g, a, acc, own, other, came, done, back, sums, last,
    in_sem, win_sem, wout_sem, m_send, m_recv, s1, r1, s2, r2, s3, r3, s4, r4, sa, ra, sb, rb,
):
    y, col, core = lax.axis_index("y"), lax.axis_index("x"), lax.axis_index("core")
    first = y * (1 - core) + col * core
    second = col * (1 - core) + y * core

    def at(i, j):
        return {"y": i * (1 - core) + j * core, "x": j * (1 - core) + i * core, "core": core}

    partner = {"core": 1 - core}
    count, width = tokens.shape
    half = width // 2
    w = half // CHUNKS
    block = 2 * count
    dist = near_first(n)
    each = n // BATCHES
    part = each * SLOTS
    group = 2 * part
    rows = each * block
    slots = n * group
    heads = n * part
    units = w_out.shape[1]

    barrier = pltpu.get_barrier_semaphore()
    for d in range(1, n):
        pl.semaphore_signal(barrier, inc=1, device_id=at((first + d) % n, second), device_id_type=MESH)
        pl.semaphore_signal(barrier, inc=1, device_id=at(first, (second + d) % n), device_id_type=MESH)
    pl.semaphore_signal(barrier, inc=1, device_id=partner, device_id_type=MESH)
    in_copies = [
        pltpu.make_async_copy(src, dst, in_sem.at[i])
        for i, (src, dst) in enumerate(
            [(tokens_in, tokens), (gain_in, gain), (ids_in, ids), (score_in, score), (pair_in, pair)])
    ]
    for copy in in_copies:
        copy.start()
    win_copies = [[
        pltpu.make_async_copy(w_in.at[0, pl.ds(h * half + k * w, w), :], win_v.at[k, h], win_sem.at[k, h])
        for h in range(2)] for k in range(CHUNKS)]
    wout_copies = [[
        pltpu.make_async_copy(w_out.at[0, :, pl.ds(h * half + k * w, w)], wout_v.at[k, h], wout_sem.at[k, h])
        for h in range(2)] for k in range(CHUNKS)]
    for copies in win_copies + wout_copies:
        for copy in copies:
            copy.start()

    for copy in in_copies:
        copy.wait()
    wide = tokens[...].astype(F32)
    scale = lax.rsqrt(jnp.mean(wide * wide, axis=-1, keepdims=True) + 1e-06)
    normed = wide * scale * gain[...]
    x[0:block, :] = jnp.concatenate([normed[:, :half], normed[:, half:]], axis=0).astype(BF16)

    scores = score[...]
    shares = (scores / jnp.sum(scores, axis=-1, keepdims=True)).astype(BF16).astype(F32)
    named = ids[...]
    experts = pair.shape[1]
    choice = lax.broadcasted_iota(jnp.int32, (count, experts), 1)
    member = jnp.zeros((count, experts), F32)
    weight = jnp.zeros((count, experts), F32)
    for k in range(named.shape[1]):
        same = choice == named[:, k:k + 1]
        member = member + jnp.where(same, 1.0, 0.0)
        weight = weight + jnp.where(same, shares[:, k:k + 1], 0.0)
    place = lax.broadcasted_iota(jnp.int32, (LANES, experts), 0)
    table = across(member.astype(BF16), jnp.where(place == pair[...], 1.0, 0.0).astype(BF16))
    row = lax.broadcasted_iota(jnp.int32, (count, LANES), 0)
    earlier = jnp.zeros((count, LANES), F32)
    for t in range(count - 1):
        earlier = earlier + jnp.where(row > t, table[t:t + 1, :], 0.0)
    table = table * (1.0 + earlier)
    table = table + across(
        weight.astype(BF16), jnp.where(place == pair[...] + HALF_LANES, 1.0, 0.0).astype(BF16))
    meta[0:block, :] = jnp.concatenate([table, table], axis=0).astype(BF16)

    pl.semaphore_wait(barrier, 2 * (n - 1) + 1)

    def block_of(q):
        return pl.ds(q * block, block)

    def group_of(p):
        return pl.ds(p * group, group)

    def send_meta(q):
        return pltpu.make_async_remote_copy(
            src_ref=meta.at[block_of(0), :], dst_ref=meta.at[block_of(q), :],
            send_sem=m_send.at[q], recv_sem=m_recv.at[q],
            device_id=at((first + dist[q]) % n, second), device_id_type=MESH)

    def send_x(k, q):
        lanes = pl.ds(k * w, w)
        return pltpu.make_async_remote_copy(
            src_ref=x.at[block_of(0), lanes], dst_ref=x.at[block_of(q), lanes],
            send_sem=s1.at[k, q], recv_sem=r1.at[k, q],
            device_id=at((first + dist[q]) % n, second), device_id_type=MESH)

    def send_slots(b, k, p):
        return pltpu.make_async_remote_copy(
            src_ref=g.at[b, k, group_of(p), :], dst_ref=a.at[b, k, group_of(p), :],
            send_sem=s2.at[b, k, p], recv_sem=r2.at[b, k, p],
            device_id=at(first, (second + p) % n), device_id_type=MESH)

    def swap_rows(b, k):
        return pltpu.make_async_remote_copy(
            src_ref=a.at[b, k, pl.ds(0, slots), :], dst_ref=a.at[b, k, pl.ds(slots, slots), :],
            send_sem=sa.at[b, k], recv_sem=ra.at[b, k], device_id=partner, device_id_type=MESH)

    def swap_partial(b, k):
        return pltpu.make_async_remote_copy(
            src_ref=other.at[b, k], dst_ref=came.at[b, k],
            send_sem=sb.at[b, k], recv_sem=rb.at[b, k], device_id=partner, device_id_type=MESH)

    def send_back(b, k, p):
        return pltpu.make_async_remote_copy(
            src_ref=done.at[b, k, group_of(p), :], dst_ref=back.at[b, k, group_of(p), :],
            send_sem=s3.at[b, k, p], recv_sem=r3.at[b, k, p],
            device_id=at(first, (second + n - p) % n), device_id_type=MESH)

    def send_sums(k, q):
        return pltpu.make_async_remote_copy(
            src_ref=sums.at[k, block_of(q), :], dst_ref=last.at[k, block_of(q), :],
            send_sem=s4.at[k, q], recv_sem=r4.at[k, q],
            device_id=at((first + n - dist[q]) % n, second), device_id_type=MESH)

    def sources(b):
        return [q for q in range(b * each, (b + 1) * each) if q > 0]

    targets = [p for p in near_first(n) if p > 0]
    for b in range(BATCHES):
        for q in sources(b):
            send_meta(q).start()
        for k in range(CHUNKS):
            for q in sources(b):
                send_x(k, q).start()

    stride = 1 + (n - 1) * core
    start = first * (n * (1 - core) + core)
    slot_a = lax.broadcasted_iota(jnp.int32, (slots, LANES), 0)
    lane_a = lax.broadcasted_iota(jnp.int32, (slots, LANES), 1)
    station = (slot_a // group + second) % n * stride + start
    choose = jnp.where(lane_a == station, 1.0, 0.0).astype(BF16)
    weigh = jnp.where(lane_a == station + HALF_LANES, 1.0, 0.0).astype(BF16)

    def matching(slot, line):
        return (slot % part // SLOTS == line // block) & (slot % group // part == line % block // count)

    slot_s = lax.broadcasted_iota(jnp.int32, (slots, rows), 0)
    match_s = matching(slot_s, lax.broadcasted_iota(jnp.int32, (slots, rows), 1))
    rank_s = (slot_s % SLOTS + 1).astype(F32)
    slot_t = lax.broadcasted_iota(jnp.int32, (rows, slots), 1)
    match_t = matching(slot_t, lax.broadcasted_iota(jnp.int32, (rows, slots), 0))
    rank_t = (slot_t % SLOTS + 1).astype(F32)

    def rows_of(b):
        return slice(b * rows, (b + 1) * rows)

    def pick_table(b):
        for q in sources(b):
            send_meta(q).wait_recv()
        return jnp.where((across(choose, meta[rows_of(b), :]) == rank_s) & match_s, 1.0, 0.0).astype(BF16)

    def mix_table(b):
        table = meta[rows_of(b), :]
        return jnp.where((across(table, choose) == rank_t) & match_t, across(table, weigh), 0.0).astype(BF16)

    def pick(b, k, picks):
        for q in sources(b):
            send_x(k, q).wait_recv()
        chosen = jnp.dot(picks, x[rows_of(b), k * w:(k + 1) * w], preferred_element_type=F32).astype(BF16)
        g[b, k] = chosen
        a[b, k, 0:group, :] = chosen[0:group]
        for p in targets:
            send_slots(b, k, p).start()

    def swap(b, k):
        for p in targets:
            send_slots(b, k, p).wait_recv()
        swap_rows(b, k).start()

    def expand(b, k):
        swap_rows(b, k).wait_recv()
        if b == 0:
            for copy in win_copies[k]:
                copy.wait()
        both = a[b, k].astype(F32).reshape(2 * n, 2, part, w)
        product = None
        for h in range(2):
            term = jnp.dot(
                both[:, h].reshape(2 * heads, w).astype(BF16), win_v[k, h], preferred_element_type=F32)
            product = term if product is None else product + term
        if k == 0:
            acc[b] = product
        else:
            acc[b] += product

    def activate(b):
        gate = acc[b, :, :units]
        return (gate / (1.0 + jnp.exp(-gate)) * acc[b, :, units:]).astype(BF16)

    def contract(b, k, hidden):
        if b == 0:
            for copy in wout_copies[k]:
                copy.wait()
        for h in range(2):
            product = jnp.dot(hidden, wout_v[k, h], preferred_element_type=F32)
            own[b, k, h] = product[:heads]
            other[b, k, h] = product[heads:].astype(BF16)
        swap_partial(b, k).start()

    def finish(b, k):
        swap_partial(b, k).wait_recv()
        total = [(own[b, k, h] + came[b, k, h].astype(F32)).reshape(n, 1, part, w) for h in range(2)]
        final = jnp.concatenate(total, axis=1).reshape(slots, w).astype(BF16)
        done[b, k] = final
        back[b, k, 0:group, :] = final[0:group]
        for p in targets:
            send_back(b, k, p).start()

    def mix(b, k, mixes):
        for p in targets:
            send_back(b, k, p).wait_recv()
        total = jnp.dot(mixes, back[b, k], preferred_element_type=F32).astype(BF16)
        sums[k, rows_of(b), :] = total
        if b == 0:
            last[k, 0:block, :] = total[0:block]
        for q in sources(b):
            send_sums(k, q).start()

    def gather(k):
        for q in range(1, n):
            send_sums(k, q).wait_recv()
        total = last[k, 0:block, :].astype(F32)
        for q in range(1, n):
            total = total + last[k, q * block:(q + 1) * block, :].astype(F32)
        for h in range(2):
            out[:, h * half + k * w:h * half + (k + 1) * w] = total[h * count:(h + 1) * count].astype(BF16)

    chunks = range(CHUNKS)
    for b in range(BATCHES):
        picks = pick_table(b)
        for k in chunks:
            pick(b, k, picks)
    mixes = [mix_table(b) for b in range(BATCHES)]
    for b in range(BATCHES):
        for stage, k in in_waves((swap, expand), CHUNKS):
            stage(b, k)
        hidden = activate(b)
        for k in chunks:
            contract(b, k, hidden)
        for k in chunks:
            if b > 0:
                mix(b - 1, k, mixes[b - 1])
            finish(b, k)
    for k in chunks:
        mix(BATCHES - 1, k, mixes[BATCHES - 1])
    for k in chunks:
        gather(k)

    for q in range(1, n):
        send_meta(q).wait_send()
        for k in chunks:
            send_x(k, q).wait_send()
            send_sums(k, q).wait_send()
    for b in range(BATCHES):
        for k in chunks:
            swap_rows(b, k).wait_send()
            swap_partial(b, k).wait_send()
            for p in targets:
                send_slots(b, k, p).wait_send()
                send_back(b, k, p).wait_send()


def in_waves(stages, chunks):
    return [
        (stages[s], wave - s)
        for wave in range(len(stages) + chunks - 1)
        for s in range(len(stages))
        if 0 <= wave - s < chunks
    ]


def on_device(tokens, norm_gain, expert_ids, route_score, expert_pair, w_in, w_out):
    n = lax.axis_size("y")
    count, width = tokens.shape
    units = w_out.shape[1]
    w = width // 2 // CHUNKS
    rows = n * 2 * count
    heads = n * (n // BATCHES) * SLOTS
    slots = 2 * heads
    experts = expert_pair.shape[0]
    vmem = pl.BlockSpec(memory_space=pltpu.VMEM)
    hbm = pl.BlockSpec(memory_space=pl.ANY)
    dma = pltpu.SemaphoreType.DMA
    return pl.pallas_call(
        functools.partial(kernel, n),
        out_shape=jax.ShapeDtypeStruct((count, width), BF16),
        in_specs=[hbm] * 7,
        out_specs=vmem,
        scratch_shapes=[
            pltpu.VMEM((count, width), BF16),
            pltpu.VMEM((1, width), F32),
            pltpu.VMEM(expert_ids.shape, jnp.int32),
            pltpu.VMEM(route_score.shape, F32),
            pltpu.VMEM((1, experts), jnp.int32),
            pltpu.VMEM((CHUNKS, 2, w, 2 * units), BF16),
            pltpu.VMEM((CHUNKS, 2, units, w), BF16),
            pltpu.VMEM((rows, width // 2), BF16),
            pltpu.VMEM((rows, LANES), BF16),
            pltpu.VMEM((BATCHES, CHUNKS, slots, w), BF16),
            pltpu.VMEM((BATCHES, CHUNKS, 2 * slots, w), BF16),
            pltpu.VMEM((BATCHES, 2 * heads, 2 * units), F32),
            pltpu.VMEM((BATCHES, CHUNKS, 2, heads, w), F32),
            pltpu.VMEM((BATCHES, CHUNKS, 2, heads, w), BF16),
            pltpu.VMEM((BATCHES, CHUNKS, 2, heads, w), BF16),
            pltpu.VMEM((BATCHES, CHUNKS, slots, w), BF16),
            pltpu.VMEM((BATCHES, CHUNKS, slots, w), BF16),
            pltpu.VMEM((CHUNKS, rows, w), BF16),
            pltpu.VMEM((CHUNKS, rows, w), BF16),
            dma((5,)), dma((CHUNKS, 2)), dma((CHUNKS, 2)), dma((n,)), dma((n,)),
            dma((CHUNKS, n)), dma((CHUNKS, n)), dma((BATCHES, CHUNKS, n)), dma((BATCHES, CHUNKS, n)),
            dma((BATCHES, CHUNKS, n)), dma((BATCHES, CHUNKS, n)), dma((CHUNKS, n)), dma((CHUNKS, n)),
            dma((BATCHES, CHUNKS)), dma((BATCHES, CHUNKS)), dma((BATCHES, CHUNKS)), dma((BATCHES, CHUNKS)),
        ],
        compiler_params=pltpu.CompilerParams(
            collective_id=0, has_side_effects=True, vmem_limit_bytes=60 << 20
        ),
    )(
        tokens, norm_gain.reshape(1, width), expert_ids, route_score, expert_pair.reshape(1, experts), w_in, w_out
    )


def solution(mesh):
    split = Mesh(mesh.devices.reshape(mesh.shape["groups"], 8, 8, 2), GROUPS_EXPERT)
    placed = (
        P(GROUPS_EXPERT, None),
        P(),
        P(GROUPS_EXPERT, None),
        P(GROUPS_EXPERT, None),
        P("groups"),
        P(GROUPS_EXPERT, None, None),
        P(GROUPS_EXPERT, None, None),
    )
    return jax.shard_map(
        on_device, mesh=split, in_specs=placed, out_specs=P(GROUPS_EXPERT, None), check_vma=False
    )
```

```python
import functools

import jax
import jax.numpy as jnp
from jax import lax
from jax.experimental import pallas as pl
from jax.experimental.pallas import tpu as pltpu
from jax.sharding import Mesh
from jax.sharding import PartitionSpec as P

MESH = pl.DeviceIdType.MESH
GROUPS_EXPERT = ("groups", "y", "x", "core")
SLOTS = 2
LANES = 128
HALF_LANES = 64
CHUNKS = 4
BATCHES = 2
F32 = jnp.float32
BF16 = jnp.bfloat16


def across(a, b):
    return lax.dot_general(a, b, (((1,), (1,)), ((), ())), preferred_element_type=F32)


def drain(ref, sem):
    pltpu.make_async_copy(ref, ref, sem).wait()


def near_first(n):
    return sorted(range(n), key=lambda d: (min(d, n - d), d))


def kernel(
    n, tokens_in, gain_in, ids_in, score_in, pair_in, w_in, w_out, out,
    tokens, gain, ids, score, pair,
    win_v, wout_v, x, meta, g, a, acc, own, other, came, done, back, sums, last,
    in_sem, win_sem, wout_sem, m_send, m_recv, s1, r1, s2, r2, s3, r3, s4, r4, sa, ra, sb, rb,
):
    y, col, core = lax.axis_index("y"), lax.axis_index("x"), lax.axis_index("core")
    first = y * (1 - core) + col * core
    second = col * (1 - core) + y * core

    def at(i, j):
        return {"y": i * (1 - core) + j * core, "x": j * (1 - core) + i * core, "core": core}

    partner = {"core": 1 - core}
    count, width = tokens.shape
    half = width // 2
    w = half // CHUNKS
    block = 2 * count
    dist = near_first(n)
    each = n // BATCHES
    part = each * SLOTS
    group = 2 * part
    rows = each * block
    slots = n * group
    heads = n * part
    units = w_out.shape[1]

    barrier = pltpu.get_barrier_semaphore()
    for d in range(1, n):
        pl.semaphore_signal(barrier, inc=1, device_id=at((first + d) % n, second), device_id_type=MESH)
        pl.semaphore_signal(barrier, inc=1, device_id=at(first, (second + d) % n), device_id_type=MESH)
    pl.semaphore_signal(barrier, inc=1, device_id=partner, device_id_type=MESH)
    in_copies = [
        pltpu.make_async_copy(src, dst, in_sem.at[i])
        for i, (src, dst) in enumerate(
            [(tokens_in, tokens), (gain_in, gain), (ids_in, ids), (score_in, score), (pair_in, pair)])
    ]
    for copy in in_copies:
        copy.start()
    win_copies = [[
        pltpu.make_async_copy(w_in.at[0, pl.ds(h * half + k * w, w), :], win_v.at[k, h], win_sem.at[k, h])
        for h in range(2)] for k in range(CHUNKS)]
    wout_copies = [[
        pltpu.make_async_copy(w_out.at[0, :, pl.ds(h * half + k * w, w)], wout_v.at[k, h], wout_sem.at[k, h])
        for h in range(2)] for k in range(CHUNKS)]
    for copies in win_copies + wout_copies:
        for copy in copies:
            copy.start()

    for copy in in_copies[:2]:
        copy.wait()
    wide = tokens[...].astype(F32)
    scale = lax.rsqrt(jnp.mean(wide * wide, axis=-1, keepdims=True) + 1e-06)
    normed = wide * scale * gain[...]
    x[0:block, :] = jnp.concatenate([normed[:, :half], normed[:, half:]], axis=0).astype(BF16)

    for copy in in_copies[2:]:
        copy.wait()
    scores = score[...]
    shares = (scores / jnp.sum(scores, axis=-1, keepdims=True)).astype(BF16).astype(F32)
    named = ids[...]
    experts = pair.shape[1]
    choice = lax.broadcasted_iota(jnp.int32, (count, experts), 1)
    member = jnp.zeros((count, experts), F32)
    weight = jnp.zeros((count, experts), F32)
    for k in range(named.shape[1]):
        same = choice == named[:, k:k + 1]
        member = member + jnp.where(same, 1.0, 0.0)
        weight = weight + jnp.where(same, shares[:, k:k + 1], 0.0)
    place = lax.broadcasted_iota(jnp.int32, (LANES, experts), 0)
    table = across(member.astype(BF16), jnp.where(place == pair[...], 1.0, 0.0).astype(BF16))
    row = lax.broadcasted_iota(jnp.int32, (count, LANES), 0)
    earlier = jnp.zeros((count, LANES), F32)
    for t in range(count - 1):
        earlier = earlier + jnp.where(row > t, table[t:t + 1, :], 0.0)
    table = table * (1.0 + earlier)
    table = table + across(
        weight.astype(BF16), jnp.where(place == pair[...] + HALF_LANES, 1.0, 0.0).astype(BF16))
    meta[0:block, :] = jnp.concatenate([table, table], axis=0).astype(BF16)

    pl.semaphore_wait(barrier, 2 * (n - 1) + 1)

    def block_of(q):
        return pl.ds(q * block, block)

    def group_of(p):
        return pl.ds(p * group, group)

    def send_meta(q):
        return pltpu.make_async_remote_copy(
            src_ref=meta.at[block_of(0), :], dst_ref=meta.at[block_of(q), :],
            send_sem=m_send, recv_sem=m_recv.at[q // each],
            device_id=at((first + dist[q]) % n, second), device_id_type=MESH)

    def send_x(k, q):
        lanes = pl.ds(k * w, w)
        return pltpu.make_async_remote_copy(
            src_ref=x.at[block_of(0), lanes], dst_ref=x.at[block_of(q), lanes],
            send_sem=s1, recv_sem=r1.at[q // each, k],
            device_id=at((first + dist[q]) % n, second), device_id_type=MESH)

    def send_slots(b, k, p):
        return pltpu.make_async_remote_copy(
            src_ref=g.at[b, k, group_of(p), :], dst_ref=a.at[b, k, group_of(p), :],
            send_sem=s2, recv_sem=r2.at[b, k],
            device_id=at(first, (second + p) % n), device_id_type=MESH)

    def swap_rows(b, k):
        return pltpu.make_async_remote_copy(
            src_ref=a.at[b, k, pl.ds(0, slots), :], dst_ref=a.at[b, k, pl.ds(slots, slots), :],
            send_sem=sa, recv_sem=ra.at[b, k], device_id=partner, device_id_type=MESH)

    def swap_partial(b, k):
        return pltpu.make_async_remote_copy(
            src_ref=other.at[b, k], dst_ref=came.at[b, k],
            send_sem=sb, recv_sem=rb.at[b, k], device_id=partner, device_id_type=MESH)

    def send_back(b, k, p):
        return pltpu.make_async_remote_copy(
            src_ref=done.at[b, k, group_of(p), :], dst_ref=back.at[b, k, group_of(p), :],
            send_sem=s3, recv_sem=r3.at[b, k],
            device_id=at(first, (second + n - p) % n), device_id_type=MESH)

    def send_sums(k, q):
        return pltpu.make_async_remote_copy(
            src_ref=sums.at[k, block_of(q), :], dst_ref=last.at[k, block_of(q), :],
            send_sem=s4, recv_sem=r4.at[k],
            device_id=at((first + n - dist[q]) % n, second), device_id_type=MESH)

    def sources(b):
        return [q for q in range(b * each, (b + 1) * each) if q > 0]

    targets = [p for p in near_first(n) if p > 0]
    for q in range(1, n):
        send_meta(q).start()
    for b in range(BATCHES):
        for k in range(CHUNKS):
            for q in sources(b):
                send_x(k, q).start()

    stride = 1 + (n - 1) * core
    start = first * (n * (1 - core) + core)
    slot_a = lax.broadcasted_iota(jnp.int32, (slots, LANES), 0)
    lane_a = lax.broadcasted_iota(jnp.int32, (slots, LANES), 1)
    station = (slot_a // group + second) % n * stride + start
    choose = jnp.where(lane_a == station, 1.0, 0.0).astype(BF16)
    weigh = jnp.where(lane_a == station + HALF_LANES, 1.0, 0.0).astype(BF16)

    def matching(slot, line):
        return (slot % part // SLOTS == line // block) & (slot % group // part == line % block // count)

    slot_s = lax.broadcasted_iota(jnp.int32, (slots, rows), 0)
    match_s = matching(slot_s, lax.broadcasted_iota(jnp.int32, (slots, rows), 1))
    rank_s = (slot_s % SLOTS + 1).astype(F32)
    slot_t = lax.broadcasted_iota(jnp.int32, (rows, slots), 1)
    match_t = matching(slot_t, lax.broadcasted_iota(jnp.int32, (rows, slots), 0))
    rank_t = (slot_t % SLOTS + 1).astype(F32)

    def rows_of(b):
        return slice(b * rows, (b + 1) * rows)

    def far_rows(b):
        low = max(b * rows, block)
        return pl.ds(low, (b + 1) * rows - low)

    others = pl.ds(group, slots - group)

    def pick_table(b):
        drain(meta.at[far_rows(b), :], m_recv.at[b])
        return jnp.where((across(choose, meta[rows_of(b), :]) == rank_s) & match_s, 1.0, 0.0).astype(BF16)

    def mix_table(b):
        table = meta[rows_of(b), :]
        return jnp.where((across(table, choose) == rank_t) & match_t, across(table, weigh), 0.0).astype(BF16)

    def pick(b, k, picks):
        drain(x.at[far_rows(b), pl.ds(k * w, w)], r1.at[b, k])
        chosen = jnp.dot(picks, x[rows_of(b), k * w:(k + 1) * w], preferred_element_type=F32).astype(BF16)
        g[b, k] = chosen
        a[b, k, 0:group, :] = chosen[0:group]
        for p in targets:
            send_slots(b, k, p).start()

    def swap(b, k):
        drain(a.at[b, k, others, :], r2.at[b, k])
        swap_rows(b, k).start()

    def expand(b, k):
        swap_rows(b, k).wait_recv()
        if b == 0:
            for copy in win_copies[k]:
                copy.wait()
        both = a[b, k].astype(F32).reshape(2 * n, 2, part, w)
        product = None
        for h in range(2):
            term = jnp.dot(
                both[:, h].reshape(2 * heads, w).astype(BF16), win_v[k, h], preferred_element_type=F32)
            product = term if product is None else product + term
        if k == 0:
            acc[b] = product
        else:
            acc[b] += product

    def activate(b):
        gate = acc[b, :, :units]
        return (gate / (1.0 + jnp.exp(-gate)) * acc[b, :, units:]).astype(BF16)

    def contract(b, k, hidden):
        if b == 0:
            for copy in wout_copies[k]:
                copy.wait()
        for h in range(2):
            product = jnp.dot(hidden, wout_v[k, h], preferred_element_type=F32)
            own[b, k, h] = product[:heads]
            other[b, k, h] = product[heads:].astype(BF16)
        swap_partial(b, k).start()

    def finish(b, k):
        swap_partial(b, k).wait_recv()
        total = [(own[b, k, h] + came[b, k, h].astype(F32)).reshape(n, 1, part, w) for h in range(2)]
        final = jnp.concatenate(total, axis=1).reshape(slots, w).astype(BF16)
        done[b, k] = final
        back[b, k, 0:group, :] = final[0:group]
        for p in targets:
            send_back(b, k, p).start()

    def mix(b, k, mixes):
        drain(back.at[b, k, others, :], r3.at[b, k])
        total = jnp.dot(mixes, back[b, k], preferred_element_type=F32).astype(BF16)
        sums[k, rows_of(b), :] = total
        if b == 0:
            last[k, 0:block, :] = total[0:block]
        for q in sources(b):
            send_sums(k, q).start()

    def gather(k):
        drain(last.at[k, pl.ds(block, (n - 1) * block), :], r4.at[k])
        total = last[k, 0:block, :].astype(F32)
        for q in range(1, n):
            total = total + last[k, q * block:(q + 1) * block, :].astype(F32)
        for h in range(2):
            out[:, h * half + k * w:h * half + (k + 1) * w] = total[h * count:(h + 1) * count].astype(BF16)

    chunks = range(CHUNKS)
    for b in range(BATCHES):
        picks = pick_table(b)
        for k in chunks:
            pick(b, k, picks)
    mixes = [mix_table(b) for b in range(BATCHES)]
    for b in range(BATCHES):
        for k in chunks:
            swap(b, k)
        for k in chunks:
            expand(b, k)
        hidden = activate(b)
        for k in chunks:
            contract(b, k, hidden)
        for k in chunks:
            finish(b, k)
    for b in range(BATCHES):
        for k in chunks:
            mix(b, k, mixes[b])
    for k in chunks:
        gather(k)

    blocks = pl.ds(block, (n - 1) * block)
    drain(meta.at[blocks, :], m_send)
    drain(x.at[blocks, :], s1)
    drain(g.at[:, :, others, :], s2)
    drain(a.at[:, :, pl.ds(0, slots), :], sa)
    drain(other, sb)
    drain(done.at[:, :, others, :], s3)
    drain(sums.at[:, blocks, :], s4)


def on_device(tokens, norm_gain, expert_ids, route_score, expert_pair, w_in, w_out):
    n = lax.axis_size("y")
    count, width = tokens.shape
    units = w_out.shape[1]
    w = width // 2 // CHUNKS
    rows = n * 2 * count
    heads = n * (n // BATCHES) * SLOTS
    slots = 2 * heads
    experts = expert_pair.shape[0]
    vmem = pl.BlockSpec(memory_space=pltpu.VMEM)
    hbm = pl.BlockSpec(memory_space=pl.ANY)
    dma = pltpu.SemaphoreType.DMA
    return pl.pallas_call(
        functools.partial(kernel, n),
        out_shape=jax.ShapeDtypeStruct((count, width), BF16),
        in_specs=[hbm] * 7,
        out_specs=vmem,
        scratch_shapes=[
            pltpu.VMEM((count, width), BF16),
            pltpu.VMEM((1, width), F32),
            pltpu.VMEM(expert_ids.shape, jnp.int32),
            pltpu.VMEM(route_score.shape, F32),
            pltpu.VMEM((1, experts), jnp.int32),
            pltpu.VMEM((CHUNKS, 2, w, 2 * units), BF16),
            pltpu.VMEM((CHUNKS, 2, units, w), BF16),
            pltpu.VMEM((rows, width // 2), BF16),
            pltpu.VMEM((rows, LANES), BF16),
            pltpu.VMEM((BATCHES, CHUNKS, slots, w), BF16),
            pltpu.VMEM((BATCHES, CHUNKS, 2 * slots, w), BF16),
            pltpu.VMEM((BATCHES, 2 * heads, 2 * units), F32),
            pltpu.VMEM((BATCHES, CHUNKS, 2, heads, w), F32),
            pltpu.VMEM((BATCHES, CHUNKS, 2, heads, w), BF16),
            pltpu.VMEM((BATCHES, CHUNKS, 2, heads, w), BF16),
            pltpu.VMEM((BATCHES, CHUNKS, slots, w), BF16),
            pltpu.VMEM((BATCHES, CHUNKS, slots, w), BF16),
            pltpu.VMEM((CHUNKS, rows, w), BF16),
            pltpu.VMEM((CHUNKS, rows, w), BF16),
            dma((5,)), dma((CHUNKS, 2)), dma((CHUNKS, 2)), dma, dma((BATCHES,)),
            dma, dma((BATCHES, CHUNKS)), dma, dma((BATCHES, CHUNKS)), dma, dma((BATCHES, CHUNKS)), dma, dma((CHUNKS,)),
            dma, dma((BATCHES, CHUNKS)), dma, dma((BATCHES, CHUNKS)),
        ],
        compiler_params=pltpu.CompilerParams(
            collective_id=0, has_side_effects=True, vmem_limit_bytes=60 << 20
        ),
    )(
        tokens, norm_gain.reshape(1, width), expert_ids, route_score, expert_pair.reshape(1, experts), w_in, w_out
    )


def solution(mesh):
    split = Mesh(mesh.devices.reshape(mesh.shape["groups"], 8, 8, 2), GROUPS_EXPERT)
    placed = (
        P(GROUPS_EXPERT, None),
        P(),
        P(GROUPS_EXPERT, None),
        P(GROUPS_EXPERT, None),
        P("groups"),
        P(GROUPS_EXPERT, None, None),
        P(GROUPS_EXPERT, None, None),
    )
    return jax.shard_map(
        on_device, mesh=split, in_specs=placed, out_specs=P(GROUPS_EXPERT, None), check_vma=False
    )
```

```python
import functools

import jax
import jax.numpy as jnp
from jax import lax
from jax.experimental import pallas as pl
from jax.experimental.pallas import tpu as pltpu
from jax.sharding import Mesh
from jax.sharding import PartitionSpec as P

MESH = pl.DeviceIdType.MESH
GROUPS_EXPERT = ("groups", "y", "x", "core")
SLOTS = 2
LANES = 128
HALF_LANES = 64
CHUNKS = 4
BATCHES = 2
LAG = 1
F32 = jnp.float32
BF16 = jnp.bfloat16


def across(a, b):
    return lax.dot_general(a, b, (((1,), (1,)), ((), ())), preferred_element_type=F32)


def drain(ref, sem):
    pltpu.make_async_copy(ref, ref, sem).wait()


def near_first(n):
    return sorted(range(n), key=lambda d: (min(d, n - d), d))


def kernel(
    n, tokens_in, gain_in, ids_in, score_in, pair_in, w_in, w_out, out,
    tokens, gain, ids, score, pair,
    win_v, wout_v, x, meta, g, a, acc, own, other, came, done, back, sums, last, far, kept, high, low,
    in_sem, win_sem, wout_sem, m_send, m_recv, s1, r1, s2, r2, s3, r3, s4, r4, sa, ra, sb, rb, s5, r5, mid_meta, mid_x,
):
    y, col, core = lax.axis_index("y"), lax.axis_index("x"), lax.axis_index("core")
    first = y * (1 - core) + col * core
    second = col * (1 - core) + y * core

    def at(i, j):
        return {"y": i * (1 - core) + j * core, "x": j * (1 - core) + i * core, "core": core}

    partner = {"core": 1 - core}
    count, width = tokens.shape
    half = width // 2
    w = half // CHUNKS
    block = 2 * count
    dist = near_first(n)
    me, high1, low1, high2, low2, high3, low3, anti = range(n)
    each = n // BATCHES
    part = each * SLOTS
    group = 2 * part
    rows = each * block
    slots = n * group
    heads = n * part
    units = w_out.shape[1]

    barrier = pltpu.get_barrier_semaphore()
    for d in range(1, n):
        pl.semaphore_signal(barrier, inc=1, device_id=at((first + d) % n, second), device_id_type=MESH)
        pl.semaphore_signal(barrier, inc=1, device_id=at(first, (second + d) % n), device_id_type=MESH)
    pl.semaphore_signal(barrier, inc=1, device_id=partner, device_id_type=MESH)
    in_copies = [
        pltpu.make_async_copy(src, dst, in_sem.at[i])
        for i, (src, dst) in enumerate(
            [(tokens_in, tokens), (gain_in, gain), (ids_in, ids), (score_in, score), (pair_in, pair)])
    ]
    for copy in in_copies:
        copy.start()
    win_copies = [[
        pltpu.make_async_copy(w_in.at[0, pl.ds(h * half + k * w, w), :], win_v.at[k, h], win_sem.at[k, h])
        for h in range(2)] for k in range(CHUNKS)]
    wout_copies = [[
        pltpu.make_async_copy(w_out.at[0, :, pl.ds(h * half + k * w, w)], wout_v.at[k, h], wout_sem.at[k, h])
        for h in range(2)] for k in range(CHUNKS)]
    for copies in win_copies + wout_copies:
        for copy in copies:
            copy.start()

    for copy in in_copies[:2]:
        copy.wait()
    wide = tokens[...].astype(F32)
    scale = lax.rsqrt(jnp.mean(wide * wide, axis=-1, keepdims=True) + 1e-06)
    normed = wide * scale * gain[...]
    x[me * block:(me + 1) * block, :] = jnp.concatenate([normed[:, :half], normed[:, half:]], axis=0).astype(BF16)

    for copy in in_copies[2:]:
        copy.wait()
    scores = score[...]
    shares = (scores / jnp.sum(scores, axis=-1, keepdims=True)).astype(BF16).astype(F32)
    named = ids[...]
    experts = pair.shape[1]
    choice = lax.broadcasted_iota(jnp.int32, (count, experts), 1)
    member = jnp.zeros((count, experts), F32)
    weight = jnp.zeros((count, experts), F32)
    for k in range(named.shape[1]):
        same = choice == named[:, k:k + 1]
        member = member + jnp.where(same, 1.0, 0.0)
        weight = weight + jnp.where(same, shares[:, k:k + 1], 0.0)
    place = lax.broadcasted_iota(jnp.int32, (LANES, experts), 0)
    table = across(member.astype(BF16), jnp.where(place == pair[...], 1.0, 0.0).astype(BF16))
    row = lax.broadcasted_iota(jnp.int32, (count, LANES), 0)
    earlier = jnp.zeros((count, LANES), F32)
    for t in range(count - 1):
        earlier = earlier + jnp.where(row > t, table[t:t + 1, :], 0.0)
    table = table * (1.0 + earlier)
    table = table + across(
        weight.astype(BF16), jnp.where(place == pair[...] + HALF_LANES, 1.0, 0.0).astype(BF16))
    meta[me * block:(me + 1) * block, :] = jnp.concatenate([table, table], axis=0).astype(BF16)

    pl.semaphore_wait(barrier, 2 * (n - 1) + 1)

    def block_of(q):
        return pl.ds(q * block, block)

    def group_of(p):
        return pl.ds(p * group, group)

    def line_copy(src, dst, send_sem, recv_sem, hop):
        return pltpu.make_async_remote_copy(
            src_ref=src, dst_ref=dst, send_sem=send_sem, recv_sem=recv_sem,
            device_id=at((first + n + hop) % n, second), device_id_type=MESH)

    def send_meta(q):
        sem = mid_meta.at[q - high2] if q >= high2 else m_recv.at[0]
        return line_copy(meta.at[block_of(me), :], meta.at[block_of(q), :], m_send, sem, dist[q])

    def pass_meta(q, to, hop):
        return line_copy(meta.at[block_of(q), :], meta.at[block_of(to), :], m_send, m_recv.at[1], hop)

    def send_x(k, q):
        lanes = pl.ds(k * w, w)
        sem = mid_x.at[q - high2, k] if q >= high2 else r1.at[0, k]
        return line_copy(x.at[block_of(me), lanes], x.at[block_of(q), lanes], s1, sem, dist[q])

    def pass_x(k, q, to, hop):
        lanes = pl.ds(k * w, w)
        return line_copy(x.at[block_of(q), lanes], x.at[block_of(to), lanes], s1, r1.at[1, k], hop)

    def send_slots(b, k, p):
        return pltpu.make_async_remote_copy(
            src_ref=g.at[b, k, group_of(p), :], dst_ref=a.at[b, k, group_of(p), :],
            send_sem=s2, recv_sem=r2.at[b, k],
            device_id=at(first, (second + p) % n), device_id_type=MESH)

    def swap_rows(b, k):
        return pltpu.make_async_remote_copy(
            src_ref=a.at[b, k, pl.ds(0, slots), :], dst_ref=a.at[b, k, pl.ds(slots, slots), :],
            send_sem=sa, recv_sem=ra.at[b, k], device_id=partner, device_id_type=MESH)

    def swap_partial(b, k):
        return pltpu.make_async_remote_copy(
            src_ref=other.at[b, k], dst_ref=came.at[b, k],
            send_sem=sb, recv_sem=rb.at[b, k], device_id=partner, device_id_type=MESH)

    def send_back(b, k, p):
        return pltpu.make_async_remote_copy(
            src_ref=done.at[b, k, group_of(p), :], dst_ref=back.at[b, k, group_of(p), :],
            send_sem=s3, recv_sem=r3.at[b, k],
            device_id=at(first, (second + n - p) % n), device_id_type=MESH)

    def send_far_sums(k, q):
        hop = {anti: -2 if k % 2 == 0 else 2, low3: 1, high3: -1}[q]
        return line_copy(sums.at[k, block_of(q), :], far.at[k, block_of(q - high3), :], s5, r5.at[k], hop)

    def send_sums(k, q):
        return line_copy(sums.at[k, block_of(q), :], last.at[k, block_of(q - high1), :], s4, r4.at[k], -dist[q])

    targets = [p for p in near_first(n) if p > 0]
    for q in (high2, low2, high1, low1):
        send_meta(q).start()
    for pair_of in ((high2, low2), (high1, low1)):
        for k in range(CHUNKS):
            for q in pair_of:
                send_x(k, q).start()
    drain(meta.at[block_of(high2), :], mid_meta.at[0])
    pass_meta(high2, high3, 1).start()
    pass_meta(high2, anti, 2).start()
    drain(meta.at[block_of(low2), :], mid_meta.at[1])
    pass_meta(low2, low3, -1).start()
    for k in range(CHUNKS):
        for q, to, step in ((high2, high3, 1), (low2, low3, -1)):
            drain(x.at[block_of(q), pl.ds(k * w, w)], mid_x.at[q - high2, k])
            pass_x(k, q, to, step).start()
            if (k % 2 == 0) == (q == high2):
                pass_x(k, q, anti, 2 * step).start()

    stride = 1 + (n - 1) * core
    start = first * (n * (1 - core) + core)
    slot_a = lax.broadcasted_iota(jnp.int32, (slots, LANES), 0)
    lane_a = lax.broadcasted_iota(jnp.int32, (slots, LANES), 1)
    station = (slot_a // group + second) % n * stride + start
    choose = jnp.where(lane_a == station, 1.0, 0.0).astype(BF16)
    weigh = jnp.where(lane_a == station + HALF_LANES, 1.0, 0.0).astype(BF16)

    def matching(slot, line):
        return (slot % part // SLOTS == line // block) & (slot % group // part == line % block // count)

    slot_s = lax.broadcasted_iota(jnp.int32, (slots, rows), 0)
    match_s = matching(slot_s, lax.broadcasted_iota(jnp.int32, (slots, rows), 1))
    rank_s = (slot_s % SLOTS + 1).astype(F32)
    slot_t = lax.broadcasted_iota(jnp.int32, (rows, slots), 1)
    match_t = matching(slot_t, lax.broadcasted_iota(jnp.int32, (rows, slots), 0))
    rank_t = (slot_t % SLOTS + 1).astype(F32)

    def rows_of(b):
        return slice(b * rows, (b + 1) * rows)

    near_blocks = pl.ds(high1 * block, 2 * block)
    far_blocks = pl.ds(high3 * block, 3 * block)
    arriving = (near_blocks, far_blocks)
    others = pl.ds(group, slots - group)

    def pick_table(b):
        drain(meta.at[arriving[b], :], m_recv.at[b])
        return jnp.where((across(choose, meta[rows_of(b), :]) == rank_s) & match_s, 1.0, 0.0).astype(BF16)

    def mix_table(b):
        table = meta[rows_of(b), :]
        return jnp.where((across(table, choose) == rank_t) & match_t, across(table, weigh), 0.0).astype(BF16)

    def pick(b, k, picks):
        drain(x.at[arriving[b], pl.ds(k * w, w)], r1.at[b, k])
        chosen = jnp.dot(picks, x[rows_of(b), k * w:(k + 1) * w], preferred_element_type=F32).astype(BF16)
        g[b, k] = chosen
        a[b, k, 0:group, :] = chosen[0:group]
        for p in targets:
            send_slots(b, k, p).start()

    def swap(b, k):
        drain(a.at[b, k, others, :], r2.at[b, k])
        swap_rows(b, k).start()

    def expand(b, k):
        swap_rows(b, k).wait_recv()
        if b == 0:
            for copy in win_copies[k]:
                copy.wait()
        both = a[b, k].astype(F32).reshape(2 * n, 2, part, w)
        product = None
        for h in range(2):
            term = jnp.dot(
                both[:, h].reshape(2 * heads, w).astype(BF16), win_v[k, h], preferred_element_type=F32)
            product = term if product is None else product + term
        if k == 0:
            acc[b] = product
        else:
            acc[b] += product

    def activate(b):
        gate = acc[b, :, :units]
        return (gate / (1.0 + jnp.exp(-gate)) * acc[b, :, units:]).astype(BF16)

    def contract(b, k, hidden):
        if b == 0:
            for copy in wout_copies[k]:
                copy.wait()
        for h in range(2):
            product = jnp.dot(hidden, wout_v[k, h], preferred_element_type=F32)
            own[b, k, h] = product[:heads]
            other[b, k, h] = product[heads:].astype(BF16)
        swap_partial(b, k).start()

    def finish(b, k):
        swap_partial(b, k).wait_recv()
        total = [(own[b, k, h] + came[b, k, h].astype(F32)).reshape(n, 1, part, w) for h in range(2)]
        final = jnp.concatenate(total, axis=1).reshape(slots, w).astype(BF16)
        done[b, k] = final
        back[b, k, 0:group, :] = final[0:group]
        for p in targets:
            send_back(b, k, p).start()

    def mix(b, k, mixes):
        drain(back.at[b, k, others, :], r3.at[b, k])
        total = jnp.dot(mixes, back[b, k], preferred_element_type=F32)
        parts = [total[i * block:(i + 1) * block] for i in range(each)]
        if b == 0:
            kept[k] = parts[me]
            high[k] = parts[high2]
            for q in (high1, low1):
                sums[k, block_of(q), :] = parts[q].astype(BF16)
                send_sums(k, q).start()
        else:
            low[k] = parts[low2 - each]
            for q in (anti, high3, low3):
                sums[k, block_of(q), :] = parts[q - each].astype(BF16)
                send_far_sums(k, q).start()

    def merge(k):
        drain(far.at[k], r5.at[k])
        over, under = high[k], low[k]
        over = over + far[k, block_of(high3 - high3), :].astype(F32)
        under = under + far[k, block_of(low3 - high3), :].astype(F32)
        if k % 2 == 0:
            over = over + far[k, block_of(anti - high3), :].astype(F32)
        else:
            under = under + far[k, block_of(anti - high3), :].astype(F32)
        for q, value in ((high2, over), (low2, under)):
            sums[k, block_of(q), :] = value.astype(BF16)
            send_sums(k, q).start()

    def gather(k):
        drain(last.at[k], r4.at[k])
        total = kept[k]
        for q in range(4):
            total = total + last[k, block_of(q), :].astype(F32)
        for h in range(2):
            out[:, h * half + k * w:h * half + (k + 1) * w] = total[h * count:(h + 1) * count].astype(BF16)

    chunks = range(CHUNKS)
    for b in range(BATCHES):
        picks = pick_table(b)
        for k in chunks:
            pick(b, k, picks)
    mixes = [mix_table(b) for b in range(BATCHES)]
    for b in range(BATCHES):
        for k in range(CHUNKS + LAG):
            if k < CHUNKS:
                swap(b, k)
            if k >= LAG:
                expand(b, k - LAG)
        hidden = activate(b)
        for k in chunks:
            contract(b, k, hidden)
        for k in chunks:
            finish(b, k)
    for b in range(BATCHES):
        for k in chunks:
            mix(b, k, mixes[b])
    for k in chunks:
        merge(k)
    for k in chunks:
        gather(k)

    drain(meta.at[pl.ds(block, (n - 1) * block), :], m_send)
    drain(x.at[pl.ds(block, (n - 1) * block), :], s1)
    drain(g.at[:, :, others, :], s2)
    drain(a.at[:, :, pl.ds(0, slots), :], sa)
    drain(other, sb)
    drain(done.at[:, :, others, :], s3)
    drain(last, s4)
    drain(far, s5)


def on_device(tokens, norm_gain, expert_ids, route_score, expert_pair, w_in, w_out):
    n = lax.axis_size("y")
    count, width = tokens.shape
    units = w_out.shape[1]
    w = width // 2 // CHUNKS
    block = 2 * count
    rows = n * block
    heads = n * (n // BATCHES) * SLOTS
    slots = 2 * heads
    experts = expert_pair.shape[0]
    vmem = pl.BlockSpec(memory_space=pltpu.VMEM)
    hbm = pl.BlockSpec(memory_space=pl.ANY)
    dma = pltpu.SemaphoreType.DMA
    return pl.pallas_call(
        functools.partial(kernel, n),
        out_shape=jax.ShapeDtypeStruct((count, width), BF16),
        in_specs=[hbm] * 7,
        out_specs=vmem,
        scratch_shapes=[
            pltpu.VMEM((count, width), BF16),
            pltpu.VMEM((1, width), F32),
            pltpu.VMEM(expert_ids.shape, jnp.int32),
            pltpu.VMEM(route_score.shape, F32),
            pltpu.VMEM((1, experts), jnp.int32),
            pltpu.VMEM((CHUNKS, 2, w, 2 * units), BF16),
            pltpu.VMEM((CHUNKS, 2, units, w), BF16),
            pltpu.VMEM((rows, width // 2), BF16),
            pltpu.VMEM((rows, LANES), BF16),
            pltpu.VMEM((BATCHES, CHUNKS, slots, w), BF16),
            pltpu.VMEM((BATCHES, CHUNKS, 2 * slots, w), BF16),
            pltpu.VMEM((BATCHES, 2 * heads, 2 * units), F32),
            pltpu.VMEM((BATCHES, CHUNKS, 2, heads, w), F32),
            pltpu.VMEM((BATCHES, CHUNKS, 2, heads, w), BF16),
            pltpu.VMEM((BATCHES, CHUNKS, 2, heads, w), BF16),
            pltpu.VMEM((BATCHES, CHUNKS, slots, w), BF16),
            pltpu.VMEM((BATCHES, CHUNKS, slots, w), BF16),
            pltpu.VMEM((CHUNKS, rows, w), BF16),
            pltpu.VMEM((CHUNKS, 4 * block, w), BF16),
            pltpu.VMEM((CHUNKS, 3 * block, w), BF16),
            pltpu.VMEM((CHUNKS, block, w), F32),
            pltpu.VMEM((CHUNKS, block, w), F32),
            pltpu.VMEM((CHUNKS, block, w), F32),
            dma((5,)), dma((CHUNKS, 2)), dma((CHUNKS, 2)), dma, dma((BATCHES,)),
            dma, dma((BATCHES, CHUNKS)), dma, dma((BATCHES, CHUNKS)), dma, dma((BATCHES, CHUNKS)), dma, dma((CHUNKS,)),
            dma, dma((BATCHES, CHUNKS)), dma, dma((BATCHES, CHUNKS)),
            dma, dma((CHUNKS,)), dma((2,)), dma((2, CHUNKS)),
        ],
        compiler_params=pltpu.CompilerParams(
            collective_id=0, has_side_effects=True, vmem_limit_bytes=60 << 20
        ),
    )(
        tokens, norm_gain.reshape(1, width), expert_ids, route_score, expert_pair.reshape(1, experts), w_in, w_out
    )


def solution(mesh):
    split = Mesh(mesh.devices.reshape(mesh.shape["groups"], 8, 8, 2), GROUPS_EXPERT)
    placed = (
        P(GROUPS_EXPERT, None),
        P(),
        P(GROUPS_EXPERT, None),
        P(GROUPS_EXPERT, None),
        P("groups"),
        P(GROUPS_EXPERT, None, None),
        P(GROUPS_EXPERT, None, None),
    )
    return jax.shard_map(
        on_device, mesh=split, in_specs=placed, out_specs=P(GROUPS_EXPERT, None), check_vma=False
    )
```

```python
import functools

import jax
import jax.numpy as jnp
from jax import lax
from jax.experimental import pallas as pl
from jax.experimental.pallas import tpu as pltpu
from jax.sharding import Mesh
from jax.sharding import PartitionSpec as P

MESH = pl.DeviceIdType.MESH
GROUPS_EXPERT = ("groups", "y", "x", "core")
SLOTS = 2
LANES = 128
HALF_LANES = 64
CHUNKS = 4
BATCHES = 2
LAG = 1
F32 = jnp.float32
BF16 = jnp.bfloat16


def across(a, b):
    return lax.dot_general(a, b, (((1,), (1,)), ((), ())), preferred_element_type=F32)


def drain(ref, sem):
    pltpu.make_async_copy(ref, ref, sem).wait()


def near_first(n):
    return sorted(range(n), key=lambda d: (min(d, n - d), d))


def kernel(
    n, tokens_in, gain_in, ids_in, score_in, pair_in, w_in, w_out, out,
    tokens, gain, ids, score, pair,
    win_v, wout_v, x, meta, g, a, acc, own, other, came, done, back, sums, last, far, kept, high, low,
    in_sem, win_sem, wout_sem, m_send, m_recv, s1, r1, s2, r2, s3, r3, s4, r4, sa, ra, sb, rb, s5, r5, mid_meta, mid_x,
):
    y, col, core = lax.axis_index("y"), lax.axis_index("x"), lax.axis_index("core")
    first = y * (1 - core) + col * core
    second = col * (1 - core) + y * core

    def at(i, j):
        return {"y": i * (1 - core) + j * core, "x": j * (1 - core) + i * core, "core": core}

    partner = {"core": 1 - core}
    count, width = tokens.shape
    half = width // 2
    w = half // CHUNKS
    block = 2 * count
    dist = near_first(n)
    me, high1, low1, high2, low2, high3, low3, anti = range(n)
    each = n // BATCHES
    part = each * SLOTS
    group = 2 * part
    rows = each * block
    slots = n * group
    heads = n * part
    units = w_out.shape[1]

    barrier = pltpu.get_barrier_semaphore()
    for d in range(1, n):
        pl.semaphore_signal(barrier, inc=1, device_id=at((first + d) % n, second), device_id_type=MESH)
        pl.semaphore_signal(barrier, inc=1, device_id=at(first, (second + d) % n), device_id_type=MESH)
    pl.semaphore_signal(barrier, inc=1, device_id=partner, device_id_type=MESH)
    in_copies = [
        pltpu.make_async_copy(src, dst, in_sem.at[i])
        for i, (src, dst) in enumerate(
            [(tokens_in, tokens), (gain_in, gain), (ids_in, ids), (score_in, score), (pair_in, pair)])
    ]
    for copy in in_copies:
        copy.start()
    win_copies = [[
        pltpu.make_async_copy(w_in.at[0, pl.ds(h * half + k * w, w), :], win_v.at[k, h], win_sem.at[k, h])
        for h in range(2)] for k in range(CHUNKS)]
    wout_copies = [[
        pltpu.make_async_copy(w_out.at[0, :, pl.ds(h * half + k * w, w)], wout_v.at[k, h], wout_sem.at[k, h])
        for h in range(2)] for k in range(CHUNKS)]
    for copies in win_copies + wout_copies:
        for copy in copies:
            copy.start()

    for copy in in_copies[:2]:
        copy.wait()
    wide = tokens[...].astype(F32)
    scale = lax.rsqrt(jnp.mean(wide * wide, axis=-1, keepdims=True) + 1e-06)
    normed = wide * scale * gain[...]
    x[me * block:(me + 1) * block, :] = jnp.concatenate([normed[:, :half], normed[:, half:]], axis=0).astype(BF16)

    for copy in in_copies[2:]:
        copy.wait()
    scores = score[...]
    shares = (scores / jnp.sum(scores, axis=-1, keepdims=True)).astype(BF16).astype(F32)
    named = ids[...]
    experts = pair.shape[1]
    choice = lax.broadcasted_iota(jnp.int32, (count, experts), 1)
    member = jnp.zeros((count, experts), F32)
    weight = jnp.zeros((count, experts), F32)
    for k in range(named.shape[1]):
        same = choice == named[:, k:k + 1]
        member = member + jnp.where(same, 1.0, 0.0)
        weight = weight + jnp.where(same, shares[:, k:k + 1], 0.0)
    place = lax.broadcasted_iota(jnp.int32, (LANES, experts), 0)
    table = across(member.astype(BF16), jnp.where(place == pair[...], 1.0, 0.0).astype(BF16))
    row = lax.broadcasted_iota(jnp.int32, (count, LANES), 0)
    earlier = jnp.zeros((count, LANES), F32)
    for t in range(count - 1):
        earlier = earlier + jnp.where(row > t, table[t:t + 1, :], 0.0)
    table = table * (1.0 + earlier)
    table = table + across(
        weight.astype(BF16), jnp.where(place == pair[...] + HALF_LANES, 1.0, 0.0).astype(BF16))
    meta[me * block:(me + 1) * block, :] = jnp.concatenate([table, table], axis=0).astype(BF16)

    pl.semaphore_wait(barrier, 2 * (n - 1) + 1)

    def block_of(q):
        return pl.ds(q * block, block)

    def group_of(p):
        return pl.ds(p * group, group)

    def line_copy(src, dst, send_sem, recv_sem, hop):
        return pltpu.make_async_remote_copy(
            src_ref=src, dst_ref=dst, send_sem=send_sem, recv_sem=recv_sem,
            device_id=at((first + n + hop) % n, second), device_id_type=MESH)

    def send_meta(q):
        sem = mid_meta.at[q - high2] if q >= high2 else m_recv.at[0]
        return line_copy(meta.at[block_of(me), :], meta.at[block_of(q), :], m_send, sem, dist[q])

    def pass_meta(q, to, hop):
        return line_copy(meta.at[block_of(q), :], meta.at[block_of(to), :], m_send, m_recv.at[1], hop)

    def send_x(k, q):
        lanes = pl.ds(k * w, w)
        sem = mid_x.at[q - high2, k] if q >= high2 else r1.at[0, k]
        return line_copy(x.at[block_of(me), lanes], x.at[block_of(q), lanes], s1, sem, dist[q])

    def pass_x(k, q, to, hop):
        lanes = pl.ds(k * w, w)
        return line_copy(x.at[block_of(q), lanes], x.at[block_of(to), lanes], s1, r1.at[1, k], hop)

    def send_slots(b, k, p):
        return pltpu.make_async_remote_copy(
            src_ref=g.at[b, k, group_of(p), :], dst_ref=a.at[b, k, group_of(p), :],
            send_sem=s2, recv_sem=r2.at[b, k],
            device_id=at(first, (second + p) % n), device_id_type=MESH)

    def swap_rows(b, k):
        return pltpu.make_async_remote_copy(
            src_ref=a.at[b, k, pl.ds(0, slots), :], dst_ref=a.at[b, k, pl.ds(slots, slots), :],
            send_sem=sa, recv_sem=ra.at[b, k], device_id=partner, device_id_type=MESH)

    def swap_partial(b, k):
        return pltpu.make_async_remote_copy(
            src_ref=other.at[b, k], dst_ref=came.at[b, k],
            send_sem=sb, recv_sem=rb.at[b, k], device_id=partner, device_id_type=MESH)

    def send_back(b, k, p):
        return pltpu.make_async_remote_copy(
            src_ref=done.at[b, k, group_of(p), :], dst_ref=back.at[b, k, group_of(p), :],
            send_sem=s3, recv_sem=r3.at[b, k],
            device_id=at(first, (second + n - p) % n), device_id_type=MESH)

    def send_far_sums(k, q):
        hop = {anti: -2 if k % 2 == 0 else 2, low3: 1, high3: -1}[q]
        return line_copy(sums.at[k, block_of(q), :], far.at[k, block_of(q - high3), :], s5, r5.at[k], hop)

    def send_sums(k, q):
        return line_copy(sums.at[k, block_of(q), :], last.at[k, block_of(q - high1), :], s4, r4.at[k], -dist[q])

    targets = [p for p in near_first(n)[::-1] if p > 0]
    for q in (high2, low2, high1, low1):
        send_meta(q).start()
    for k in range(CHUNKS):
        for q in (high2, low2, high1, low1):
            send_x(k, q).start()
    drain(meta.at[block_of(high2), :], mid_meta.at[0])
    pass_meta(high2, high3, 1).start()
    pass_meta(high2, anti, 2).start()
    drain(meta.at[block_of(low2), :], mid_meta.at[1])
    pass_meta(low2, low3, -1).start()
    def relay(k):
        for q, to, step in ((high2, high3, 1), (low2, low3, -1)):
            drain(x.at[block_of(q), pl.ds(k * w, w)], mid_x.at[q - high2, k])
            pass_x(k, q, to, step).start()
            if (k % 2 == 0) == (q == high2):
                pass_x(k, q, anti, 2 * step).start()

    stride = 1 + (n - 1) * core
    start = first * (n * (1 - core) + core)
    slot_a = lax.broadcasted_iota(jnp.int32, (slots, LANES), 0)
    lane_a = lax.broadcasted_iota(jnp.int32, (slots, LANES), 1)
    station = (slot_a // group + second) % n * stride + start
    choose = jnp.where(lane_a == station, 1.0, 0.0).astype(BF16)
    weigh = jnp.where(lane_a == station + HALF_LANES, 1.0, 0.0).astype(BF16)

    def matching(slot, line):
        return (slot % part // SLOTS == line // block) & (slot % group // part == line % block // count)

    slot_s = lax.broadcasted_iota(jnp.int32, (slots, rows), 0)
    match_s = matching(slot_s, lax.broadcasted_iota(jnp.int32, (slots, rows), 1))
    rank_s = (slot_s % SLOTS + 1).astype(F32)
    slot_t = lax.broadcasted_iota(jnp.int32, (rows, slots), 1)
    match_t = matching(slot_t, lax.broadcasted_iota(jnp.int32, (rows, slots), 0))
    rank_t = (slot_t % SLOTS + 1).astype(F32)

    def rows_of(b):
        return slice(b * rows, (b + 1) * rows)

    near_blocks = pl.ds(high1 * block, 2 * block)
    far_blocks = pl.ds(high3 * block, 3 * block)
    arriving = (near_blocks, far_blocks)
    others = pl.ds(group, slots - group)

    def pick_table(b):
        drain(meta.at[arriving[b], :], m_recv.at[b])
        return jnp.where((across(choose, meta[rows_of(b), :]) == rank_s) & match_s, 1.0, 0.0).astype(BF16)

    def mix_table(b):
        table = meta[rows_of(b), :]
        return jnp.where((across(table, choose) == rank_t) & match_t, across(table, weigh), 0.0).astype(BF16)

    def pick(b, k, picks):
        drain(x.at[arriving[b], pl.ds(k * w, w)], r1.at[b, k])
        chosen = jnp.dot(picks, x[rows_of(b), k * w:(k + 1) * w], preferred_element_type=F32).astype(BF16)
        g[b, k] = chosen
        a[b, k, 0:group, :] = chosen[0:group]
        for p in targets:
            send_slots(b, k, p).start()

    def swap(b, k):
        drain(a.at[b, k, others, :], r2.at[b, k])
        swap_rows(b, k).start()

    def expand(b, k):
        swap_rows(b, k).wait_recv()
        if b == 0:
            for copy in win_copies[k]:
                copy.wait()
        both = a[b, k].astype(F32).reshape(2 * n, 2, part, w)
        product = None
        for h in range(2):
            term = jnp.dot(
                both[:, h].reshape(2 * heads, w).astype(BF16), win_v[k, h], preferred_element_type=F32)
            product = term if product is None else product + term
        if k == 0:
            acc[b] = product
        else:
            acc[b] += product

    def activate(b):
        gate = acc[b, :, :units]
        return (gate / (1.0 + jnp.exp(-gate)) * acc[b, :, units:]).astype(BF16)

    def contract(b, k, hidden):
        if b == 0:
            for copy in wout_copies[k]:
                copy.wait()
        for h in range(2):
            product = jnp.dot(hidden, wout_v[k, h], preferred_element_type=F32)
            own[b, k, h] = product[:heads]
            other[b, k, h] = product[heads:].astype(BF16)
        swap_partial(b, k).start()

    def finish(b, k):
        swap_partial(b, k).wait_recv()
        total = [(own[b, k, h] + came[b, k, h].astype(F32)).reshape(n, 1, part, w) for h in range(2)]
        final = jnp.concatenate(total, axis=1).reshape(slots, w).astype(BF16)
        done[b, k] = final
        back[b, k, 0:group, :] = final[0:group]
        for p in targets:
            send_back(b, k, p).start()

    def mix(b, k, mixes):
        drain(back.at[b, k, others, :], r3.at[b, k])
        total = jnp.dot(mixes, back[b, k], preferred_element_type=F32)
        parts = [total[i * block:(i + 1) * block] for i in range(each)]
        if b == 0:
            kept[k] = parts[me]
            high[k] = parts[high2]
            for q in (high1, low1):
                sums[k, block_of(q), :] = parts[q].astype(BF16)
                send_sums(k, q).start()
        else:
            low[k] = parts[low2 - each]
            for q in (anti, high3, low3):
                sums[k, block_of(q), :] = parts[q - each].astype(BF16)
                send_far_sums(k, q).start()

    def merge(k):
        drain(far.at[k], r5.at[k])
        over, under = high[k], low[k]
        over = over + far[k, block_of(high3 - high3), :].astype(F32)
        under = under + far[k, block_of(low3 - high3), :].astype(F32)
        if k % 2 == 0:
            over = over + far[k, block_of(anti - high3), :].astype(F32)
        else:
            under = under + far[k, block_of(anti - high3), :].astype(F32)
        for q, value in ((high2, over), (low2, under)):
            sums[k, block_of(q), :] = value.astype(BF16)
            send_sums(k, q).start()

    def gather(k):
        drain(last.at[k], r4.at[k])
        total = kept[k]
        for q in range(4):
            total = total + last[k, block_of(q), :].astype(F32)
        for h in range(2):
            out[:, h * half + k * w:h * half + (k + 1) * w] = total[h * count:(h + 1) * count].astype(BF16)

    chunks = range(CHUNKS)
    for b in range(BATCHES):
        picks = pick_table(b)
        for k in chunks:
            if b == 0:
                relay(k)
            pick(b, k, picks)
    mixes = [mix_table(b) for b in range(BATCHES)]
    for b in range(BATCHES):
        for k in range(CHUNKS + LAG):
            if k < CHUNKS:
                swap(b, k)
            if k >= LAG:
                expand(b, k - LAG)
        hidden = activate(b)
        for k in chunks:
            contract(b, k, hidden)
        for k in chunks:
            finish(b, k)
    for b in range(BATCHES):
        for k in chunks:
            mix(b, k, mixes[b])
    for k in chunks:
        merge(k)
    for k in chunks:
        gather(k)

    drain(meta.at[pl.ds(block, (n - 1) * block), :], m_send)
    drain(x.at[pl.ds(block, (n - 1) * block), :], s1)
    drain(g.at[:, :, others, :], s2)
    drain(a.at[:, :, pl.ds(0, slots), :], sa)
    drain(other, sb)
    drain(done.at[:, :, others, :], s3)
    drain(last, s4)
    drain(far, s5)


def on_device(tokens, norm_gain, expert_ids, route_score, expert_pair, w_in, w_out):
    n = lax.axis_size("y")
    count, width = tokens.shape
    units = w_out.shape[1]
    w = width // 2 // CHUNKS
    block = 2 * count
    rows = n * block
    heads = n * (n // BATCHES) * SLOTS
    slots = 2 * heads
    experts = expert_pair.shape[0]
    vmem = pl.BlockSpec(memory_space=pltpu.VMEM)
    hbm = pl.BlockSpec(memory_space=pltpu.HBM)
    dma = pltpu.SemaphoreType.DMA
    return pl.pallas_call(
        functools.partial(kernel, n),
        out_shape=jax.ShapeDtypeStruct((count, width), BF16),
        in_specs=[hbm] * 7,
        out_specs=vmem,
        scratch_shapes=[
            pltpu.VMEM((count, width), BF16),
            pltpu.VMEM((1, width), F32),
            pltpu.VMEM(expert_ids.shape, jnp.int32),
            pltpu.VMEM(route_score.shape, F32),
            pltpu.VMEM((1, experts), jnp.int32),
            pltpu.VMEM((CHUNKS, 2, w, 2 * units), BF16),
            pltpu.VMEM((CHUNKS, 2, units, w), BF16),
            pltpu.VMEM((rows, width // 2), BF16),
            pltpu.VMEM((rows, LANES), BF16),
            pltpu.VMEM((BATCHES, CHUNKS, slots, w), BF16),
            pltpu.VMEM((BATCHES, CHUNKS, 2 * slots, w), BF16),
            pltpu.VMEM((BATCHES, 2 * heads, 2 * units), F32),
            pltpu.VMEM((BATCHES, CHUNKS, 2, heads, w), F32),
            pltpu.VMEM((BATCHES, CHUNKS, 2, heads, w), BF16),
            pltpu.VMEM((BATCHES, CHUNKS, 2, heads, w), BF16),
            pltpu.VMEM((BATCHES, CHUNKS, slots, w), BF16),
            pltpu.VMEM((BATCHES, CHUNKS, slots, w), BF16),
            pltpu.VMEM((CHUNKS, rows, w), BF16),
            pltpu.VMEM((CHUNKS, 4 * block, w), BF16),
            pltpu.VMEM((CHUNKS, 3 * block, w), BF16),
            pltpu.VMEM((CHUNKS, block, w), F32),
            pltpu.VMEM((CHUNKS, block, w), F32),
            pltpu.VMEM((CHUNKS, block, w), F32),
            dma((5,)), dma((CHUNKS, 2)), dma((CHUNKS, 2)), dma, dma((BATCHES,)),
            dma, dma((BATCHES, CHUNKS)), dma, dma((BATCHES, CHUNKS)), dma, dma((BATCHES, CHUNKS)), dma, dma((CHUNKS,)),
            dma, dma((BATCHES, CHUNKS)), dma, dma((BATCHES, CHUNKS)),
            dma, dma((CHUNKS,)), dma((2,)), dma((2, CHUNKS)),
        ],
        compiler_params=pltpu.CompilerParams(
            collective_id=0, has_side_effects=True, vmem_limit_bytes=40 << 20
        ),
    )(
        *[
            pltpu.with_memory_space_constraint(v, pltpu.HBM)
            for v in (
                tokens, norm_gain.reshape(1, width), expert_ids, route_score, expert_pair.reshape(1, experts), w_in, w_out
            )
        ]
    )


def solution(mesh):
    split = Mesh(mesh.devices.reshape(mesh.shape["groups"], 8, 8, 2), GROUPS_EXPERT)
    placed = (
        P(GROUPS_EXPERT, None),
        P(),
        P(GROUPS_EXPERT, None),
        P(GROUPS_EXPERT, None),
        P("groups"),
        P(GROUPS_EXPERT, None, None),
        P(GROUPS_EXPERT, None, None),
    )
    return jax.shard_map(
        on_device, mesh=split, in_specs=placed, out_specs=P(GROUPS_EXPERT, None), check_vma=False
    )
```
